1024 devices in a mesh: row: 32 (over y_lo, z), col: 32 (over x, y_hi, core).
Axes of the slice: x: 4, y: 8 (y_hi: 4, y_lo: 2; y = y_hi * 2 + y_lo), z: 16, core: 2. Of those that a mesh axis runs over, the one named last changes fastest.
Arguments:
- hidden: bfloat16 [2048, 4096], P('row'), may hold values from -6 to 6
- queries: bfloat16 [2048, 64, 128], P(('row', 'col')), may hold values from -6 to 6
- keys: bfloat16 [2048, 4, 64, 128], P(('row', 'col')), may hold values from -6 to 6
- values: bfloat16 [2048, 4, 64, 128], P(('row', 'col')), may hold values from -12 to 12
- out_proj: bfloat16 [8192, 4096], P('col'), may hold values from -0.0625 to 0.0625
- norm_gain: float32 [4096], replicated, may hold values from 0.4 to 1.6
- routes: int32 [2048, 8], P('row'), may hold values from 0 to 127, all different within a row; in each aligned block of 64 rows (0 to 63, 64 to 127, ...) at most 8 rows name the same one
- route_probs: float32 [2048, 8], P('row'), may hold values from 0.05 to 1
- w_gate: bfloat16 [4096, 131072], P(None, ('row', 'col')), may hold values from -0.09375 to 0.09375
- w_up: bfloat16 [4096, 131072], P(None, ('row', 'col')), may hold values from -0.09375 to 0.09375
- w_down: bfloat16 [131072, 4096], P(('row', 'col')), may hold values from -0.1875 to 0.1875
Outputs:
- updated: bfloat16 [2048, 4096], P(('row', 'col'))
The draws below stay inside these ranges and needn't reach their ends.
Inputs may be any that keep to these rules, and one draw needn't show every extreme that they name: `routes`: each row names 8 different experts. In each aligned block of 64 rows (the requests of one index of row) no expert is named by more than 8 rows.
All inputs are finite; a program needn't handle non-finite values.
Results may differ from the reference program's by a relative error of at most 0.017.
Values may be sent and summed in bfloat16 or wider, within the bound.
No kernel may reach another device: no remote copies, remote signals or barrier semaphores. Data moves between devices by JAX's collectives and lax.ppermute only.
A program may use at most 32 MiB of HBM per device.

```python
import math
import jax
import jax.numpy as jnp
import numpy as np
from jax import lax

D = 4096
HEADS = 64
KVH = 4
HD = 128
EXPERTS = 128
TOP = 8
FF = 1024
LEN = 64
TOKENS = 2048
BLOCK = 64
CAP = 8
N_ROW = 32
DEVICES = 1024


def shared_attention(key):
    base = jax.random.fold_in(key, 7)
    query_key, cache_key = jax.random.split(base, 2)
    query_draw = jnp.clip(jax.random.normal(query_key, (TOKENS, HEADS, HD), jnp.float32), -4.0, 4.0)
    cache_draw = jnp.clip(jax.random.normal(cache_key, (TOKENS, KVH, LEN, HD), jnp.float32), -4.0, 4.0)
    return (query_draw, cache_draw)


def draw_queries(key, part):
    return shared_attention(key)[0].astype(jnp.bfloat16)


def draw_keys(key, part):
    return shared_attention(key)[1].astype(jnp.bfloat16)


def level_of(key, dims, cuts, least, largest):
    factor_of = 1.0
    for axis_at, blocks in cuts:
        heights = jax.random.uniform(jax.random.fold_in(jax.random.fold_in(key, 6), axis_at), (blocks,), jnp.float32, least / len(cuts), largest / len(cuts))
        factor_of = factor_of * jnp.repeat(jnp.exp(heights), dims[axis_at] // blocks).reshape((-1,) + (1,) * (len(dims) - 1 - axis_at))
    return factor_of


def assign_block(key, own, number, rows, amount, top, bound, lean):
    sequence = jax.random.permutation(key, amount)
    crowded, common = load_shares(amount, rows * top, bound, lean, True), load_shares(amount, rows * top, bound, lean, False)
    places = jnp.arange(amount)

    def named(lengths, rotation):
        used = int((lengths > 0).sum())
        fixed = max(1, used // 4)
        passed = fixed + (places - fixed + rotation * (used - fixed)) % max(1, amount - fixed)
        return jnp.zeros((amount,), jnp.int32).at[sequence[jnp.where(places < fixed, places, passed)]].set(jnp.asarray(lengths, jnp.int32))

    lengths = jnp.where(number % 4 == 0, named(crowded, number // 4), named(common, number - number // 4 - 1))
    mixed = jax.random.permutation(jax.random.fold_in(own, 3), amount)
    giver, sink = mixed[0:amount // 2 * 2:2], mixed[1:amount // 2 * 2:2]
    room = jnp.minimum(lengths[giver] - 1, bound - lengths[sink]) // 2
    room = jnp.where((giver == sequence[0]) | (sink == sequence[0]) | (lengths[sink] == 0), 0, jnp.maximum(room, 0))
    passed = jax.random.randint(jax.random.fold_in(own, 4), (amount // 2,), 0, 1 << 20) % (room + 1)
    lengths = lengths.at[giver].add(-passed).at[sink].add(passed)
    labels = jnp.searchsorted(jnp.cumsum(lengths), jnp.arange(rows * top), side="right").astype(jnp.int32)
    grid = labels.reshape(top, rows).T
    grid = grid[jax.random.permutation(jax.random.fold_in(own, 1), rows)]
    rotation = jax.random.randint(jax.random.fold_in(own, 2), (rows, 1), 0, top)
    return jnp.take_along_axis(grid, (jnp.arange(top)[None, :] + rotation) % top, axis=1)


def load_shares(number_of, total, bound, lean, full):
    portions = [(1 << 20) // math.isqrt(grade ** lean) + 1 for grade in range(1, number_of + 1)]
    largest = bound if full else min(bound, max(-(-total // number_of), total * portions[0] // sum(portions)))
    least = 1 if total - largest >= number_of - 1 else 0
    counts, spare = [largest] + [least] * (number_of - 1), total - largest - least * (number_of - 1)
    while spare > 0:
        free = [i for i in range(1, number_of) if counts[i] < largest] or [i for i in range(1, number_of) if counts[i] < bound]
        whole, budget = sum([portions[i] for i in free]), spare
        for i in free:
            extra = min(bound - counts[i], max(1, budget * portions[i] // whole), spare)
            counts[i] = counts[i] + extra
            spare = spare - extra
    return np.array(counts)


def noise(own_key, shape, width, limit, shards=(), kind=jnp.bfloat16):
    loudness = level_of(own_key, shape, shards, -0.22, 0.18) if shards else 1.0
    entries = jax.random.normal(own_key, shape, jnp.float32) * width * loudness
    return jnp.minimum(jnp.maximum(entries, -limit), limit).astype(kind)


def setup_inputs(seed: int = 0) -> dict:
    splits = jax.random.split(jax.random.key(seed), 12)
    hidden = noise(splits[0], (TOKENS, D), 1.0, 6.0, ((0, 32),))
    queries = draw_queries(jax.random.fold_in(splits[11], 71), 0)
    keys = draw_keys(jax.random.fold_in(splits[11], 71), 0)
    values = noise(splits[3], (TOKENS, KVH, LEN, HD), 2.0, 12.0, ((0, 1024),))
    out_proj = noise(splits[4], (HEADS * HD, D), (HEADS * HD) ** -0.5, 0.0625, ((0, 32),))
    norm_gain = jnp.clip(1.0 + 0.12 * jax.random.normal(splits[5], (D,), jnp.float32), 0.4, 1.6)
    routes_keys = jax.random.split(jax.random.fold_in(splits[6], 1), TOKENS // BLOCK)
    routes_turns = jax.random.permutation(jax.random.fold_in(splits[6], 3), TOKENS // BLOCK)
    routes = jax.vmap(lambda own, number: assign_block(jax.random.fold_in(splits[6], 2), own, number, BLOCK, EXPERTS, TOP, CAP, 2))(routes_keys, routes_turns).reshape((TOKENS, TOP))
    route_probs = jnp.clip(jnp.exp(math.log(1.0) - 2.9957323 * jax.random.uniform(splits[7], (TOKENS, TOP), jnp.float32) ** level_of(splits[7], (TOKENS, TOP), ((0, 32),), -0.2, 0.2)), 0.05, 1.0)
    w_gate = noise(splits[8], (D, EXPERTS * FF), D ** -0.5, 0.09375, ((1, 1024),))
    w_up = noise(splits[9], (D, EXPERTS * FF), D ** -0.5, 0.09375, ((1, 1024),))
    w_down = noise(splits[10], (EXPERTS * FF, D), FF ** -0.5, 0.1875, ((0, 1024),))
    return dict(hidden=hidden, queries=queries, keys=keys, values=values, out_proj=out_proj, norm_gain=norm_gain, routes=routes, route_probs=route_probs, w_gate=w_gate, w_up=w_up, w_down=w_down)


def normalize(resid, norm_gain):
    mean_square = lax.optimization_barrier(jnp.mean(resid * resid, axis=-1, keepdims=True))
    return (resid * lax.rsqrt(mean_square + 1e-06) * norm_gain).astype(jnp.bfloat16)

def reference(hidden, queries, keys, values, out_proj, norm_gain, routes, route_probs, w_gate, w_up, w_down):
    group = HEADS // KVH
    grouped = queries.astype(jnp.float32).reshape(TOKENS, KVH, group, HD)
    scores = jnp.einsum('tgqd,tgpd->tgqp', grouped, keys.astype(jnp.float32)) / math.sqrt(HD)
    attn_weights = jax.nn.softmax(scores, axis=-1).astype(jnp.bfloat16)
    context = jnp.einsum('tgqp,tgpd->tgqd', attn_weights.astype(jnp.float32), values.astype(jnp.float32))
    context = context.astype(jnp.bfloat16).reshape(TOKENS, HEADS * HD)
    attn = jnp.dot(context, out_proj, preferred_element_type=jnp.float32)
    resid = hidden.astype(jnp.float32) + attn
    normed = normalize(resid, norm_gain)
    route_weight = (route_probs / lax.optimization_barrier(jnp.sum(route_probs, axis=-1, keepdims=True))).astype(jnp.bfloat16)
    hid_dev = EXPERTS * FF // DEVICES
    slice_width = min(FF, hid_dev)
    pieces = FF // slice_width
    blocks = normed.reshape(N_ROW, BLOCK, D).astype(jnp.float32)
    slot_ids = jnp.arange(CAP, dtype=jnp.int32)

    def one_expert(total, expert):
        match = routes == expert
        hits = jnp.any(match, axis=-1).astype(jnp.int32).reshape(N_ROW, BLOCK)
        chosen = lax.optimization_barrier(jnp.sum(jnp.where(match, route_weight.astype(jnp.float32), 0.0), axis=-1)).reshape(N_ROW, BLOCK)
        before = jnp.cumsum(hits, axis=1) - hits
        place = ((hits[:, None, :] == 1) & (before[:, None, :] == slot_ids[None, :, None])).astype(jnp.float32)
        arrived = jnp.einsum('rkt,rtd->rkd', place, blocks).astype(jnp.bfloat16).astype(jnp.float32)
        gate_cols = lax.dynamic_slice_in_dim(w_gate, expert * FF, FF, 1).astype(jnp.float32)
        up_cols = lax.dynamic_slice_in_dim(w_up, expert * FF, FF, 1).astype(jnp.float32)
        gate = jnp.einsum('rkd,df->rkf', arrived, gate_cols)
        upward = jnp.einsum('rkd,df->rkf', arrived, up_cols)
        act = (jax.nn.silu(gate) * upward).astype(jnp.bfloat16).astype(jnp.float32)
        act = act.reshape(N_ROW, CAP, pieces, slice_width)
        down_rows = lax.dynamic_slice_in_dim(w_down, expert * FF, FF, 0).astype(jnp.float32)
        down_rows = down_rows.reshape(pieces, slice_width, D)
        piece = jnp.einsum('rkse,sed->rksd', act, down_rows).astype(jnp.bfloat16).astype(jnp.float32)
        scaled = place * chosen[:, None, :]
        added = jnp.einsum('rkt,rksd->rtd', scaled, piece)
        return (total + added, None)
    start = jnp.zeros((N_ROW, BLOCK, D), jnp.float32)
    total, _ = lax.scan(one_expert, start, jnp.arange(EXPERTS, dtype=jnp.int32))
    mixture = total.reshape(TOKENS, D)
    return (resid + mixture).astype(jnp.bfloat16)
```

```python
import math

import jax
import jax.numpy as jnp
from jax import lax
from jax.sharding import Mesh, PartitionSpec as P

CAP = 8
NX, NY, NC = 4, 4, 2
COL = ("x", "yhi", "core")
F32 = jnp.float32
BF16 = jnp.bfloat16


def exchange(value, axis):
    return lax.all_to_all(value, axis, 0, 0, tiled=True)


def shift(value, axis, step):
    n = lax.axis_size(axis)
    return lax.ppermute(value, axis, [(i, (i + step) % n) for i in range(n)])


def attention(queries, keys, values):
    tok, heads, hd = queries.shape
    kv = keys.shape[1]
    grouped = queries.reshape(tok, kv, heads // kv, hd)
    scores = jnp.einsum(
        "tgqd,tgpd->tgqp", grouped, keys, preferred_element_type=F32
    ) / math.sqrt(hd)
    attn_weights = jax.nn.softmax(scores, axis=-1).astype(BF16)
    context = jnp.einsum("tgqp,tgpd->tgqd", attn_weights, values, preferred_element_type=F32)
    return context.astype(BF16).reshape(tok, heads * hd)


def shards(
    hidden, queries, keys, values, out_proj, norm_gain, routes, route_probs, w_gate, w_up, w_down
):
    rows = lax.axis_size("row")
    x, yhi, core = lax.axis_index("x"), lax.axis_index("yhi"), lax.axis_index("core")
    col_id = (x * NY + yhi) * NC + core
    tok_dev = queries.shape[0]
    block, d_model = hidden.shape
    wide = d_model // (NY * NC)
    mine = (yhi * NC + core) * wide

    context = attention(queries, keys, values)
    cols = NX * NY * NC
    heads_out = jnp.moveaxis(context.reshape(tok_dev, cols, -1), 1, 0)
    head_rows = exchange(heads_out, COL).reshape(block, -1)

    part = jnp.dot(head_rows, out_proj, preferred_element_type=F32).reshape(block, NY, NC, wide)
    even, odd = part[:, :, 0], part[:, :, 1]
    theirs = jnp.where(core == 0, odd, even).astype(BF16)
    ours = jnp.where(core == 0, even, odd)
    pair = ours + shift(theirs, "core", 1).astype(F32)
    quarter = exchange(jnp.moveaxis(pair.astype(BF16), 1, 0), "yhi")
    quarter = jnp.sum(quarter.astype(F32), axis=0).astype(BF16)
    every = exchange(jnp.broadcast_to(quarter[None], (NX, block, wide)), "x")
    attn = jnp.sum(every.astype(F32), axis=0)
    resid = lax.dynamic_slice_in_dim(hidden, mine, wide, 1).astype(F32) + attn
    resid16 = resid.astype(BF16)

    experts = jnp.arange(rows, dtype=jnp.int32) * NX + x
    match = routes.T[None, :, :] == experts[:, None, None]
    hits = jnp.any(match, axis=1)
    route_weight = (route_probs / jnp.sum(route_probs, axis=-1, keepdims=True)).astype(BF16)
    chosen = jnp.sum(jnp.where(match, route_weight.T[None], jnp.zeros((), BF16)), axis=1)
    earlier = jnp.arange(block)[:, None] < jnp.arange(block)[None, :]
    before = jnp.dot(hits.astype(BF16), earlier.astype(BF16), preferred_element_type=F32)
    slots = jnp.arange(CAP, dtype=F32)
    place = hits[:, None, :] & (before[:, None, :] == slots[None, :, None])
    place = place.astype(BF16)
    scaled = place * chosen[:, None, :]

    outgoing = jnp.einsum("rkt,td->rkd", place, resid16, preferred_element_type=F32).astype(BF16)
    arrived = exchange(outgoing, "row")
    count = rows * CAP
    half = count // 2
    own = arrived.reshape(count, wide)
    lo, hi = own[:half], own[half:]

    left0 = shift(lo, "yhi", 1)
    right1 = shift(hi, "yhi", -1)
    left1 = shift(hi, "yhi", 1)
    right0 = shift(lo, "yhi", -1)
    far0 = shift(left0, "yhi", 1)
    far1 = shift(right1, "yhi", -1)
    right = jnp.concatenate([right0, right1], 0)
    far = jnp.concatenate([far0, far1], 0)
    left = jnp.concatenate([left0, left1], 0)
    same = [own, right, far, left]
    other = [shift(p, "core", 1) for p in same]

    def offset(step, flip):
        c = (core + flip) % NC
        return (((yhi + step) % NY) * NC + c) * wide

    gain = norm_gain[:, None]
    gate_w = (w_gate.astype(F32) * gain).astype(BF16)
    up_w = (w_up.astype(F32) * gain).astype(BF16)
    gate = up = squares = None
    for flip, pieces in enumerate((same, other)):
        for step, piece in enumerate(pieces):
            at = offset(step, flip)
            g = jnp.dot(
                piece, lax.dynamic_slice_in_dim(gate_w, at, wide, 0), preferred_element_type=F32
            )
            u = jnp.dot(
                piece, lax.dynamic_slice_in_dim(up_w, at, wide, 0), preferred_element_type=F32
            )
            wide_piece = piece.astype(F32)
            q = jnp.sum(wide_piece * wide_piece, axis=1, keepdims=True)
            gate = g if gate is None else gate + g
            up = u if up is None else up + u
            squares = q if squares is None else squares + q
    inv = lax.rsqrt(squares / d_model + 1e-06)
    act = (jax.nn.silu(gate * inv) * (up * inv)).astype(BF16)

    def down(step, flip):
        w = lax.dynamic_slice_in_dim(w_down, offset(step, flip), wide, 1)
        return jnp.dot(act, w, preferred_element_type=F32)

    def summed(step):
        sent = shift(down(step, 1).astype(BF16), "core", 1)
        return down(step, 0) + sent.astype(F32)

    far, right, left, own = summed(2), summed(1), summed(3), summed(0)
    from_left = shift(far[:half].astype(BF16), "yhi", 1)
    from_right = shift(far[half:].astype(BF16), "yhi", -1)
    left_hi = shift(right[half:].astype(BF16), "yhi", 1)
    right_lo = shift(left[:half].astype(BF16), "yhi", -1)
    left_lo = shift((right[:half] + from_left.astype(F32)).astype(BF16), "yhi", 1)
    right_hi = shift((left[half:] + from_right.astype(F32)).astype(BF16), "yhi", -1)
    low = own[:half] + left_lo.astype(F32) + right_lo.astype(F32)
    high = own[half:] + left_hi.astype(F32) + right_hi.astype(F32)
    back = jnp.concatenate([low, high], 0).astype(BF16).reshape(rows, CAP, wide)
    returned = exchange(back, "row")

    mixed = jnp.einsum("rkt,rkd->td", scaled, returned, preferred_element_type=F32)
    mixed = mixed + jnp.where(x == 0, attn, 0.0)
    final = exchange(mixed.astype(BF16).reshape(cols, tok_dev, wide), COL)
    final = jnp.sum(final.astype(F32).reshape(NX, NY * NC, tok_dev, wide), axis=0)
    final = jnp.moveaxis(final, 0, 1).reshape(tok_dev, d_model)
    own_hidden = lax.dynamic_slice_in_dim(hidden, col_id * tok_dev, tok_dev, 0)
    return (own_hidden.astype(F32) + final).astype(BF16)


def solution(mesh):
    rows = mesh.shape["row"]
    fine = Mesh(mesh.devices.reshape(rows, NX, NY, NC), ("row",) + COL)
    every = ("row",) + COL
    return jax.shard_map(
        shards,
        mesh=fine,
        in_specs=(
            P("row", None),
            P(every, None, None),
            P(every, None, None, None),
            P(every, None, None, None),
            P(COL, None),
            P(),
            P("row", None),
            P("row", None),
            P(None, every),
            P(None, every),
            P(every, None),
        ),
        out_specs=P(every, None),
        check_vma=False,
    )
```

```python
import math

import jax
import jax.numpy as jnp
from jax import lax
from jax.experimental import pallas as pl
from jax.experimental.pallas import tpu as pltpu
from jax.sharding import Mesh, PartitionSpec as P

CAP = 8
NX, NY, NC = 4, 4, 2
COL = ("x", "yhi", "core")
F32 = jnp.float32
BF16 = jnp.bfloat16


def exchange(value, axis):
    return lax.all_to_all(value, axis, 0, 0, tiled=True)


def swap_cores(value):
    return lax.ppermute(value, "core", [(i, (i + 1) % NC) for i in range(NC)])


def turn(value, step):
    return lax.ppermute(value, "yhi", [(i, (i + step) % NY) for i in range(NY)])


def to_all(value, axis, length):
    return exchange(jnp.broadcast_to(value[None], (length, *value.shape)), axis)


def attention(queries, keys, values):
    tok, heads, hd = queries.shape
    kv = keys.shape[1]
    grouped = queries.reshape(tok, kv, heads // kv, hd)
    scores = jnp.einsum(
        "tgqd,tgpd->tgqp", grouped, keys, preferred_element_type=F32
    ) / math.sqrt(hd)
    attn_weights = jax.nn.softmax(scores, axis=-1).astype(BF16)
    context = jnp.einsum("tgqp,tgpd->tgqd", attn_weights, values, preferred_element_type=F32)
    return context.astype(BF16).reshape(tok, heads * hd)


def hidden_units(place_ref, own_ref, other_ref, gain_ref, wg_ref, wu_ref, act_ref):
    pieces, count, wide = own_ref.shape
    step = 2 * wide
    steps = pieces // 2
    total = jnp.zeros((count, 2 * wg_ref.shape[1]), F32)
    squares = jnp.zeros((count, step), F32)
    for flip, ref in enumerate((own_ref, other_ref)):
        first = ((place_ref[0] + flip) % NC) * steps
        for p in range(steps):
            rows = jnp.concatenate([ref[2 * p], ref[2 * p + 1]], axis=1).astype(F32)
            squares = squares + rows * rows
            scaled = (rows * gain_ref[pl.ds(first + p, 1), :]).astype(BF16)
            at = pl.multiple_of((first + p) * step, step)
            both = jnp.concatenate([wg_ref[pl.ds(at, step), :], wu_ref[pl.ds(at, step), :]], axis=1)
            total = total + jnp.dot(scaled, both, preferred_element_type=F32)
    features = 2 * steps * step
    inv = lax.rsqrt(jnp.sum(squares, axis=1, keepdims=True) / features + 1e-06)
    gate = total[:, : wg_ref.shape[1]] * inv
    up = total[:, wg_ref.shape[1] :] * inv
    act_ref[...] = (gate / (1.0 + jnp.exp(-gate)) * up).astype(BF16)


def down_rows(place_ref, own_ref, other_ref, wd0_ref, wd1_ref, wd2_ref, wd3_ref, out_ref):
    total = jnp.zeros(out_ref.shape, F32)
    for step, wd_ref in enumerate((wd0_ref, wd1_ref, wd2_ref, wd3_ref)):
        y = (place_ref[1] + NY - step) % NY
        for flip, ref in enumerate((own_ref, other_ref)):
            total = total + jnp.dot(ref[y], wd_ref[flip], preferred_element_type=F32)
    out_ref[...] = total.astype(BF16)


def project(h_ref, w_ref, out_ref):
    cols, _, thin = out_ref.shape
    half = cols // NC
    for core in range(NC):
        for p in range(0, half, 2):
            at = (core * half + p) * thin
            both = jnp.dot(
                h_ref[...], w_ref[:, at : at + 2 * thin], preferred_element_type=F32
            ).astype(BF16)
            out_ref[p * NC + core] = both[:, :thin]
            out_ref[(p + 1) * NC + core] = both[:, thin:]


def cut_features(place_ref, w_ref, same_ref, other_ref):
    thin = same_ref.shape[2] // NX
    for flip, ref in enumerate((same_ref, other_ref)):
        core = (place_ref[0] + flip) % NC
        for step in range(NY):
            y = (place_ref[1] + step) % NY
            for x in range(NX):
                at = pl.multiple_of(((core * NX + x) * NY + y) * thin, thin)
                ref[step, :, x * thin : (x + 1) * thin] = w_ref[:, pl.ds(at, thin)]


def spread(in_ref, out_ref):
    rows, slots, thin = in_ref.shape
    per = slots // NX
    for x in range(NX):
        piece = in_ref[:, x * per : (x + 1) * per, :].reshape(rows * per, thin)
        for y in range(NY):
            out_ref[x * NY + y] = piece


def local_call(body, outs, n_in, scalars=False):
    vmem = pl.BlockSpec(memory_space=pltpu.VMEM)
    head = [pl.BlockSpec(memory_space=pltpu.SMEM)] if scalars else []
    out_shape = [jax.ShapeDtypeStruct(shape, BF16) for shape in outs]
    single = len(outs) == 1
    return pl.pallas_call(
        body,
        out_shape=out_shape[0] if single else out_shape,
        in_specs=head + [vmem] * n_in,
        out_specs=vmem if single else [vmem] * len(outs),
        compiler_params=pltpu.CompilerParams(vmem_limit_bytes=24 * 1024 * 1024),
    )


def shards(
    hidden, queries, keys, values, out_proj, norm_gain, routes, route_probs, w_gate, w_up, w_down
):
    rows = lax.axis_size("row")
    x, yhi, core = lax.axis_index("x"), lax.axis_index("yhi"), lax.axis_index("core")
    col_id = (x * NY + yhi) * NC + core
    tok_dev = queries.shape[0]
    block, d_model = hidden.shape
    cols = NX * NY * NC
    thin = d_model // cols
    wide = d_model // (NY * NC)
    count = rows * CAP
    place_at = jnp.stack([core, yhi]).astype(jnp.int32)

    route_weight = (route_probs / jnp.sum(route_probs, axis=-1, keepdims=True)).astype(BF16)
    earlier = (jnp.arange(block)[:, None] < jnp.arange(block)[None, :]).astype(BF16)
    slots = jnp.arange(CAP, dtype=F32)

    def slotted(experts):
        match = routes.T[None, :, :] == experts[:, None, None]
        hits = jnp.any(match, axis=1)
        before = jnp.dot(hits.astype(BF16), earlier, preferred_element_type=F32)
        place = hits[:, None, :] & (before[:, None, :] == slots[None, :, None])
        return match, place.astype(BF16)

    _, place = slotted(jnp.arange(rows * NX, dtype=jnp.int32))
    place = place.reshape(rows * NX * CAP, block)
    match, mine = slotted(jnp.arange(rows, dtype=jnp.int32) * NX + x)
    chosen = jnp.sum(jnp.where(match, route_weight.T[None], jnp.zeros((), BF16)), axis=1)
    combine = (mine * chosen[:, None, :]).reshape(count, block).T

    context = attention(queries, keys, values)
    heads_out = jnp.moveaxis(context.reshape(tok_dev, cols, -1), 1, 0)
    head_rows = exchange(heads_out, COL).reshape(block, -1)

    part = local_call(project, [(cols, block, thin)], 2)(head_rows, out_proj)
    attn = jnp.sum(exchange(part, COL).astype(F32), axis=0)
    own_at = ((core * NX + x) * NY + yhi) * thin
    resid = lax.dynamic_slice_in_dim(hidden, own_at, thin, 1).astype(F32) + attn

    outgoing = jnp.dot(place, resid.astype(BF16), preferred_element_type=F32).astype(BF16)
    arrived = exchange(outgoing.reshape(rows, NX * CAP, thin), "row")

    hid = w_down.shape[0]
    same, rest = local_call(cut_features, [(NY, hid, wide)] * 2, 1, True)(place_at, w_down)
    pieces = [jnp.stack(pair) for pair in zip(same, swap_cores(rest))]
    down = [pieces[0]] + [turn(pieces[step], step) for step in (1, 3, 2)]
    down = [down[0], down[1], down[3], down[2]]

    by_expert = local_call(spread, [(NX * NY, count, thin)], 1)(arrived)
    own = exchange(by_expert, ("x", "yhi"))
    other = swap_cores(own)

    act = local_call(hidden_units, [(count, w_gate.shape[1])], 5, True)(
        place_at, own, other, norm_gain.reshape(-1, 2 * thin), w_gate, w_up
    )
    own_act = to_all(act, "yhi", NY)
    other_act = swap_cores(own_act)
    back = local_call(down_rows, [(count, wide)], 6, True)(place_at, own_act, other_act, *down)
    returned = exchange(back.reshape(rows, CAP, wide), "row").reshape(count, wide)

    attn_here = jnp.concatenate([jnp.where(x == i, attn, 0.0) for i in range(NX)], axis=1)
    mixed = jnp.dot(combine, returned, preferred_element_type=F32) + attn_here
    final = exchange(mixed.astype(BF16).reshape(cols, tok_dev, wide), COL)
    final = jnp.sum(final.astype(F32).reshape(NX, NY, NC, tok_dev, NX, thin), axis=0)
    final = jnp.transpose(final, (2, 1, 3, 0, 4)).reshape(tok_dev, d_model)
    own_hidden = lax.dynamic_slice_in_dim(hidden, col_id * tok_dev, tok_dev, 0)
    return (own_hidden.astype(F32) + final).astype(BF16)


def solution(mesh):
    rows = mesh.shape["row"]
    fine = Mesh(mesh.devices.reshape(rows, NX, NY, NC), ("row",) + COL)
    every = ("row",) + COL
    return jax.shard_map(
        shards,
        mesh=fine,
        in_specs=(
            P("row", None),
            P(every, None, None),
            P(every, None, None, None),
            P(every, None, None, None),
            P(COL, None),
            P(),
            P("row", None),
            P("row", None),
            P(None, every),
            P(None, every),
            P(every, None),
        ),
        out_specs=P(every, None),
        check_vma=False,
    )
```

```python
import math

import jax
import jax.numpy as jnp
from jax import lax
from jax.experimental import pallas as pl
from jax.experimental.pallas import tpu as pltpu
from jax.sharding import Mesh, PartitionSpec as P

CAP = 8
NX, NY, NC = 4, 4, 2
COL = ("x", "yhi", "core")
F32 = jnp.float32
BF16 = jnp.bfloat16


def exchange(value, axis):
    return lax.all_to_all(value, axis, 0, 0, tiled=True)


def swap_cores(value):
    return lax.ppermute(value, "core", [(i, (i + 1) % NC) for i in range(NC)])


def turn(value, step):
    return lax.ppermute(value, "yhi", [(i, (i + step) % NY) for i in range(NY)])


def to_all(value, axis, length):
    return exchange(jnp.broadcast_to(value[None], (length, *value.shape)), axis)


def attention(queries, keys, values):
    tok, heads, hd = queries.shape
    kv = keys.shape[1]
    grouped = queries.reshape(tok, kv, heads // kv, hd)
    scores = jnp.einsum(
        "tgqd,tgpd->tgqp", grouped, keys, preferred_element_type=F32
    ) / math.sqrt(hd)
    attn_weights = jax.nn.softmax(scores, axis=-1).astype(BF16)
    context = jnp.einsum("tgqp,tgpd->tgqd", attn_weights, values, preferred_element_type=F32)
    return context.astype(BF16).reshape(tok, heads * hd)


def hidden_units(rows_ref, gain_ref, wg0_ref, wg1_ref, wu0_ref, wu1_ref, act_ref):
    _, count, thin = rows_ref.shape
    hid = wg0_ref.shape[1]
    step = 2 * thin
    steps = gain_ref.shape[0]
    total = jnp.zeros((count, 4 * hid), F32)
    squares = jnp.zeros((count, step), F32)
    for at in range(steps):
        core, pair = divmod(at, steps // NC)
        first = 2 * pair * NC + core
        rows = jnp.concatenate([rows_ref[first], rows_ref[first + NC]], axis=1).astype(F32)
        squares = squares + rows * rows
        scaled = (rows * gain_ref[at : at + 1, :]).astype(BF16)
        here = slice(at * step, (at + 1) * step)
        weights = jnp.concatenate(
            [wg0_ref[here, :], wg1_ref[here, :], wu0_ref[here, :], wu1_ref[here, :]], axis=1
        )
        total = total + jnp.dot(scaled, weights, preferred_element_type=F32)
    inv = lax.rsqrt(jnp.sum(squares, axis=1, keepdims=True) / (steps * step) + 1e-06)
    gate = total[:, : 2 * hid] * inv
    up = total[:, 2 * hid :] * inv
    act_ref[...] = (gate / (1.0 + jnp.exp(-gate)) * up).astype(BF16)


def down_rows(own_ref, other_ref, wd0_ref, wd1_ref, wd2_ref, wd3_ref, out_ref):
    core, yhi = lax.axis_index("core"), lax.axis_index("yhi")
    half = own_ref.shape[1]
    for flip, ref in enumerate((own_ref, other_ref)):
        total = jnp.zeros((half, out_ref.shape[1]), F32)
        for step, wd_ref in enumerate((wd0_ref, wd1_ref, wd2_ref, wd3_ref)):
            act = ref[lax.rem(yhi + NY - step, NY)]
            weights = jnp.concatenate([wd_ref[flip], wd_ref[1 - flip]], axis=0)
            total = total + jnp.dot(act, weights, preferred_element_type=F32)
        at = pl.multiple_of(lax.rem(core + flip, NC) * half, half)
        out_ref[pl.ds(at, half), :] = total.astype(BF16)


def project(h_ref, w0_ref, w1_ref, out_ref):
    thin = out_ref.shape[2]
    for core, w_ref in enumerate((w0_ref, w1_ref)):
        both = jnp.dot(h_ref[...], w_ref[...], preferred_element_type=F32).astype(BF16)
        out_ref[core] = both[:, :thin]
        out_ref[NC + core] = both[:, thin:]


def projected(head_rows, out_proj, cols, thin):
    block, depth = head_rows.shape
    steps = cols // NC // 2
    return pl.pallas_call(
        project,
        grid=(steps,),
        out_shape=jax.ShapeDtypeStruct((cols, block, thin), BF16),
        in_specs=[
            pl.BlockSpec((block, depth), lambda g: (0, 0)),
            pl.BlockSpec((depth, 2 * thin), lambda g: (0, g)),
            pl.BlockSpec((depth, 2 * thin), lambda g: (0, g + steps)),
        ],
        out_specs=pl.BlockSpec((2 * NC, block, thin), lambda g: (g, 0, 0)),
    )(head_rows, out_proj, out_proj)


def cut_features(w_ref, same_ref, other_ref):
    core, yhi = lax.axis_index("core"), lax.axis_index("yhi")
    thin = same_ref.shape[2] // NX
    for flip, ref in enumerate((same_ref, other_ref)):
        c = lax.rem(core + flip, NC)
        for step in range(NY):
            y = lax.rem(yhi + step, NY)
            for x in range(NX):
                at = pl.multiple_of(((c * NX + x) * NY + y) * thin, thin)
                ref[step, :, x * thin : (x + 1) * thin] = w_ref[:, pl.ds(at, thin)]


def spread(in_ref, out_ref):
    rows, slots, thin = in_ref.shape
    per, half = slots // NX, rows // NC
    for x in range(NX):
        for core in range(NC):
            part = in_ref[core * half : (core + 1) * half, x * per : (x + 1) * per, :]
            part = part.reshape(half * per, thin)
            for y in range(NY):
                out_ref[(x * NY + y) * NC + core] = part


def join(in_ref, hidden_ref, out_ref):
    _, _, wide = in_ref.shape
    thin = wide // NX
    for y in range(NY):
        for core in range(NC):
            total = in_ref[y * NC + core].astype(F32)
            for x in range(1, NX):
                total = total + in_ref[(x * NY + y) * NC + core].astype(F32)
            for x in range(NX):
                at = ((core * NX + x) * NY + y) * thin
                here = slice(at, at + thin)
                done = total[:, x * thin : (x + 1) * thin] + hidden_ref[:, here].astype(F32)
                out_ref[:, here] = done.astype(BF16)


def local_call(body, outs, n_in):
    vmem = pl.BlockSpec(memory_space=pltpu.VMEM)
    out_shape = [jax.ShapeDtypeStruct(shape, BF16) for shape in outs]
    single = len(outs) == 1
    return pl.pallas_call(
        body,
        out_shape=out_shape[0] if single else out_shape,
        in_specs=[vmem] * n_in,
        out_specs=vmem if single else [vmem] * len(outs),
        compiler_params=pltpu.CompilerParams(vmem_limit_bytes=24 * 1024 * 1024),
    )


def shards(
    hidden, queries, keys, values, out_proj, norm_gain, routes, route_probs, w_gate, w_up, w_down
):
    rows = lax.axis_size("row")
    x, yhi, core = lax.axis_index("x"), lax.axis_index("yhi"), lax.axis_index("core")
    col_id = (x * NY + yhi) * NC + core
    tok_dev = queries.shape[0]
    block, d_model = hidden.shape
    cols = NX * NY * NC
    thin = d_model // cols
    wide = d_model // (NY * NC)
    count = rows * CAP

    route_weight = (route_probs / jnp.sum(route_probs, axis=-1, keepdims=True)).astype(BF16)
    earlier = (jnp.arange(block)[:, None] < jnp.arange(block)[None, :]).astype(BF16)
    slots = jnp.arange(CAP, dtype=F32)

    def slotted(experts):
        match = routes.T[None, :, :] == experts[:, None, None]
        hits = jnp.any(match, axis=1)
        before = jnp.dot(hits.astype(BF16), earlier, preferred_element_type=F32)
        place = hits[:, None, :] & (before[:, None, :] == slots[None, :, None])
        return match, place.astype(BF16)

    _, place = slotted(jnp.arange(rows * NX, dtype=jnp.int32))
    place = place.reshape(rows * NX * CAP, block)
    match, mine = slotted(jnp.arange(rows, dtype=jnp.int32) * NX + x)
    chosen = jnp.sum(jnp.where(match, route_weight.T[None], jnp.zeros((), BF16)), axis=1)
    combine = (mine * chosen[:, None, :]).reshape(count, block).T

    gate_other, up_other = swap_cores(w_gate), swap_cores(w_up)

    context = attention(queries, keys, values)
    heads_out = jnp.moveaxis(context.reshape(tok_dev, cols, -1), 1, 0)
    head_rows = exchange(heads_out, COL).reshape(block, -1)

    part = projected(head_rows, out_proj, cols, thin)
    attn = jnp.sum(exchange(part, COL).astype(F32), axis=0)
    own_at = ((core * NX + x) * NY + yhi) * thin
    resid = lax.dynamic_slice_in_dim(hidden, own_at, thin, 1).astype(F32) + attn

    outgoing = jnp.dot(place, resid.astype(BF16), preferred_element_type=F32).astype(BF16)
    arrived = exchange(outgoing.reshape(rows, NX * CAP, thin), "row")

    hid = w_down.shape[0]
    same, rest = local_call(cut_features, [(NY, hid, wide)] * 2, 1)(w_down)
    pieces = [jnp.stack(pair) for pair in zip(same, swap_cores(rest))]
    down = [pieces[0]] + [turn(pieces[step], step) for step in (1, 3, 2)]
    down = [down[0], down[1], down[3], down[2]]

    by_expert = local_call(spread, [(cols, count // NC, thin)], 1)(arrived)
    features = exchange(by_expert, COL)
    act = local_call(hidden_units, [(count // NC, NC * hid)], 6)(
        features, norm_gain.reshape(-1, 2 * thin), w_gate, gate_other, w_up, up_other
    )
    own_act = to_all(act, "yhi", NY)
    other_act = swap_cores(own_act)
    back = local_call(down_rows, [(count, wide)], 6)(own_act, other_act, *down)
    returned = exchange(back.reshape(rows, CAP, wide), "row").reshape(count, wide)

    own_hidden = lax.dynamic_slice_in_dim(hidden, col_id * tok_dev, tok_dev, 0)
    own_hidden, returned = lax.optimization_barrier((own_hidden, returned))

    attn_here = jnp.concatenate([jnp.where(x == i, attn, 0.0) for i in range(NX)], axis=1)
    mixed = jnp.dot(combine, returned, preferred_element_type=F32) + attn_here
    final = exchange(mixed.astype(BF16).reshape(cols, tok_dev, wide), COL)
    return local_call(join, [(tok_dev, d_model)], 2)(final, own_hidden)


def solution(mesh):
    rows = mesh.shape["row"]
    fine = Mesh(mesh.devices.reshape(rows, NX, NY, NC), ("row",) + COL)
    every = ("row",) + COL
    return jax.shard_map(
        shards,
        mesh=fine,
        in_specs=(
            P("row", None),
            P(every, None, None),
            P(every, None, None, None),
            P(every, None, None, None),
            P(COL, None),
            P(),
            P("row", None),
            P("row", None),
            P(None, every),
            P(None, every),
            P(every, None),
        ),
        out_specs=P(every, None),
        check_vma=False,
    )
```

```python
import math

import jax
import jax.numpy as jnp
from jax import lax
from jax.experimental import pallas as pl
from jax.experimental.pallas import tpu as pltpu
from jax.sharding import Mesh, PartitionSpec as P

CAP = 8
NX, NY, NC = 4, 4, 2
COL = ("x", "yhi", "core")
F32 = jnp.float32
BF16 = jnp.bfloat16


def exchange(value, axis):
    return lax.all_to_all(value, axis, 0, 0, tiled=True)


def swap_cores(value):
    return lax.ppermute(value, "core", [(i, (i + 1) % NC) for i in range(NC)])


def turn(value, step):
    return lax.ppermute(value, "yhi", [(i, (i + step) % NY) for i in range(NY)])


def to_all(value, axis, length):
    return exchange(jnp.broadcast_to(value[None], (length, *value.shape)), axis)


def attention(queries, keys, values):
    tok, heads, hd = queries.shape
    kv = keys.shape[1]
    grouped = queries.reshape(tok, kv, heads // kv, hd)
    scores = jnp.einsum(
        "tgqd,tgpd->tgqp", grouped, keys, preferred_element_type=F32
    ) / math.sqrt(hd)
    attn_weights = jax.nn.softmax(scores, axis=-1).astype(BF16)
    context = jnp.einsum("tgqp,tgpd->tgqd", attn_weights, values, preferred_element_type=F32)
    return context.astype(BF16).reshape(tok, heads * hd)


def hidden_units(rows_ref, gain_ref, wg0_ref, wg1_ref, wu0_ref, wu1_ref, act_ref):
    _, count, thin = rows_ref.shape
    hid = wg0_ref.shape[1]
    step = 2 * thin
    steps = gain_ref.shape[0]
    total = jnp.zeros((count, 4 * hid), F32)
    squares = jnp.zeros((count, step), F32)
    for at in range(steps):
        core, pair = divmod(at, steps // NC)
        first = 2 * pair * NC + core
        rows = jnp.concatenate([rows_ref[first], rows_ref[first + NC]], axis=1).astype(F32)
        squares = squares + rows * rows
        scaled = (rows * gain_ref[at : at + 1, :]).astype(BF16)
        here = slice(at * step, (at + 1) * step)
        weights = jnp.concatenate(
            [wg0_ref[here, :], wg1_ref[here, :], wu0_ref[here, :], wu1_ref[here, :]], axis=1
        )
        total = total + jnp.dot(scaled, weights, preferred_element_type=F32)
    inv = lax.rsqrt(jnp.sum(squares, axis=1, keepdims=True) / (steps * step) + 1e-06)
    gate = total[:, : 2 * hid] * inv
    up = total[:, 2 * hid :] * inv
    act_ref[...] = (gate / (1.0 + jnp.exp(-gate)) * up).astype(BF16)


def down_rows(own_ref, other_ref, wd0_ref, wd1_ref, wd2_ref, wd3_ref, out_ref):
    core, yhi = lax.axis_index("core"), lax.axis_index("yhi")
    half = own_ref.shape[1]
    for flip, ref in enumerate((own_ref, other_ref)):
        total = jnp.zeros((half, out_ref.shape[1]), F32)
        for step, wd_ref in enumerate((wd0_ref, wd1_ref, wd2_ref, wd3_ref)):
            act = ref[lax.rem(yhi + NY - step, NY)]
            weights = jnp.concatenate([wd_ref[flip], wd_ref[1 - flip]], axis=0)
            total = total + jnp.dot(act, weights, preferred_element_type=F32)
        at = pl.multiple_of(lax.rem(core + flip, NC) * half, half)
        out_ref[pl.ds(at, half), :] = total.astype(BF16)


CHUNKS = 4


def project(h_ref, w_ref, out_ref, held, sems):
    thin = out_ref.shape[2]
    chunk = held.shape[2]
    half = out_ref.shape[0] // NC
    copies = [
        pltpu.make_async_copy(w_ref.at[:, pl.ds(i * chunk, chunk)], held.at[i], sems.at[i])
        for i in range(CHUNKS)
    ]
    for copy in copies:
        copy.start()
    rows = h_ref[...]
    for i, copy in enumerate(copies):
        copy.wait()
        for at in range(0, chunk, 2 * thin):
            both = jnp.dot(
                rows, held[i, :, at : at + 2 * thin], preferred_element_type=F32
            ).astype(BF16)
            core, p = divmod((i * chunk + at) // thin, half)
            out_ref[p * NC + core] = both[:, :thin]
            out_ref[(p + 1) * NC + core] = both[:, thin:]


def projected(head_rows, out_proj, cols, thin):
    block, depth = head_rows.shape
    vmem = pl.BlockSpec(memory_space=pltpu.VMEM)
    return pl.pallas_call(
        project,
        out_shape=jax.ShapeDtypeStruct((cols, block, thin), BF16),
        in_specs=[vmem, pl.BlockSpec(memory_space=pl.ANY)],
        out_specs=vmem,
        scratch_shapes=[
            pltpu.VMEM((CHUNKS, depth, cols * thin // CHUNKS), BF16),
            pltpu.SemaphoreType.DMA((CHUNKS,)),
        ],
    )(head_rows, out_proj)


def cut_features(w_ref, same_ref, other_ref):
    core, yhi = lax.axis_index("core"), lax.axis_index("yhi")
    thin = same_ref.shape[2] // NX
    for flip, ref in enumerate((same_ref, other_ref)):
        c = lax.rem(core + flip, NC)
        for step in range(NY):
            y = lax.rem(yhi + step, NY)
            for x in range(NX):
                at = pl.multiple_of(((c * NX + x) * NY + y) * thin, thin)
                ref[step, :, x * thin : (x + 1) * thin] = w_ref[:, pl.ds(at, thin)]


def spread(in_ref, out_ref):
    rows, slots, thin = in_ref.shape
    per, half = slots // NX, rows // NC
    for x in range(NX):
        for core in range(NC):
            part = in_ref[core * half : (core + 1) * half, x * per : (x + 1) * per, :]
            part = part.reshape(half * per, thin)
            for y in range(NY):
                out_ref[(x * NY + y) * NC + core] = part


def join(in_ref, hidden_ref, out_ref):
    _, _, wide = in_ref.shape
    thin = wide // NX
    for y in range(NY):
        for core in range(NC):
            total = in_ref[y * NC + core].astype(F32)
            for x in range(1, NX):
                total = total + in_ref[(x * NY + y) * NC + core].astype(F32)
            for x in range(NX):
                at = ((core * NX + x) * NY + y) * thin
                here = slice(at, at + thin)
                done = total[:, x * thin : (x + 1) * thin] + hidden_ref[:, here].astype(F32)
                out_ref[:, here] = done.astype(BF16)


def local_call(body, outs, n_in):
    vmem = pl.BlockSpec(memory_space=pltpu.VMEM)
    out_shape = [jax.ShapeDtypeStruct(shape, BF16) for shape in outs]
    single = len(outs) == 1
    return pl.pallas_call(
        body,
        out_shape=out_shape[0] if single else out_shape,
        in_specs=[vmem] * n_in,
        out_specs=vmem if single else [vmem] * len(outs),
        compiler_params=pltpu.CompilerParams(vmem_limit_bytes=24 * 1024 * 1024),
    )


def shards(
    hidden, queries, keys, values, out_proj, norm_gain, routes, route_probs, w_gate, w_up, w_down
):
    rows = lax.axis_size("row")
    x, yhi, core = lax.axis_index("x"), lax.axis_index("yhi"), lax.axis_index("core")
    col_id = (x * NY + yhi) * NC + core
    tok_dev = queries.shape[0]
    block, d_model = hidden.shape
    cols = NX * NY * NC
    thin = d_model // cols
    wide = d_model // (NY * NC)
    count = rows * CAP

    route_weight = (route_probs / jnp.sum(route_probs, axis=-1, keepdims=True)).astype(BF16)
    earlier = (jnp.arange(block)[:, None] < jnp.arange(block)[None, :]).astype(BF16)
    slots = jnp.arange(CAP, dtype=F32)

    def slotted(experts):
        match = routes.T[None, :, :] == experts[:, None, None]
        hits = jnp.any(match, axis=1)
        before = jnp.dot(hits.astype(BF16), earlier, preferred_element_type=F32)
        place = hits[:, None, :] & (before[:, None, :] == slots[None, :, None])
        return match, place.astype(BF16)

    _, place = slotted(jnp.arange(rows * NX, dtype=jnp.int32))
    place = place.reshape(rows * NX * CAP, block)
    match, mine = slotted(jnp.arange(rows, dtype=jnp.int32) * NX + x)
    chosen = jnp.sum(jnp.where(match, route_weight.T[None], jnp.zeros((), BF16)), axis=1)
    combine = (mine * chosen[:, None, :]).reshape(count, block).T

    gate_other, up_other = swap_cores(w_gate), swap_cores(w_up)

    context = attention(queries, keys, values)
    heads_out = jnp.moveaxis(context.reshape(tok_dev, cols, -1), 1, 0)
    head_rows = exchange(heads_out, COL).reshape(block, -1)

    part = projected(head_rows, out_proj, cols, thin)
    part = exchange(part, COL)
    attn = jnp.sum(part.astype(F32), axis=0)
    own_at = ((core * NX + x) * NY + yhi) * thin
    place, hidden_part = lax.optimization_barrier(
        (place, lax.dynamic_slice_in_dim(hidden, own_at, thin, 1))
    )
    resid = hidden_part.astype(F32) + attn

    outgoing = jnp.dot(place, resid.astype(BF16), preferred_element_type=F32).astype(BF16)
    arrived = exchange(outgoing.reshape(rows, NX * CAP, thin), "row")

    hid = w_down.shape[0]
    same, rest = local_call(cut_features, [(NY, hid, wide)] * 2, 1)(w_down)
    rest = swap_cores(rest)
    pieces = [jnp.stack(pair) for pair in zip(same, rest)]
    down = [pieces[0]] + [turn(pieces[step], step) for step in (1, 3, 2)]
    down = [down[0], down[1], down[3], down[2]]

    by_expert = local_call(spread, [(cols, count // NC, thin)], 1)(arrived)
    features = exchange(by_expert, COL)
    act = local_call(hidden_units, [(count // NC, NC * hid)], 6)(
        features, norm_gain.reshape(-1, 2 * thin), w_gate, gate_other, w_up, up_other
    )
    own_act = to_all(act, "yhi", NY)
    other_act = swap_cores(own_act)
    back = local_call(down_rows, [(count, wide)], 6)(own_act, other_act, *down)
    returned = exchange(back.reshape(rows, CAP, wide), "row").reshape(count, wide)

    own_hidden = lax.dynamic_slice_in_dim(hidden, col_id * tok_dev, tok_dev, 0)
    own_hidden, returned = lax.optimization_barrier((own_hidden, returned))

    attn_here = jnp.concatenate([jnp.where(x == i, attn, 0.0) for i in range(NX)], axis=1)
    mixed = jnp.dot(combine, returned, preferred_element_type=F32) + attn_here
    final = exchange(mixed.astype(BF16).reshape(cols, tok_dev, wide), COL)
    return local_call(join, [(tok_dev, d_model)], 2)(final, own_hidden)


def solution(mesh):
    rows = mesh.shape["row"]
    fine = Mesh(mesh.devices.reshape(rows, NX, NY, NC), ("row",) + COL)
    every = ("row",) + COL
    return jax.shard_map(
        shards,
        mesh=fine,
        in_specs=(
            P("row", None),
            P(every, None, None),
            P(every, None, None, None),
            P(every, None, None, None),
            P(COL, None),
            P(),
            P("row", None),
            P("row", None),
            P(None, every),
            P(None, every),
            P(every, None),
        ),
        out_specs=P(every, None),
        check_vma=False,
    )
```

```python
import math

import jax
import jax.numpy as jnp
from jax import lax
from jax.experimental import pallas as pl
from jax.experimental.pallas import tpu as pltpu
from jax.sharding import Mesh, PartitionSpec as P

CAP = 8
NX, NY, NC = 4, 4, 2
COL = ("x", "yhi", "core")
F32 = jnp.float32
BF16 = jnp.bfloat16


def exchange(value, axis):
    return lax.all_to_all(value, axis, 0, 0, tiled=True)


def swap_cores(value):
    return lax.ppermute(value, "core", [(i, (i + 1) % NC) for i in range(NC)])


def turn(value, step):
    return lax.ppermute(value, "yhi", [(i, (i + step) % NY) for i in range(NY)])


def to_all(value, axis, length):
    return exchange(jnp.broadcast_to(value[None], (length, *value.shape)), axis)


def attention(queries, keys, values):
    tok, heads, hd = queries.shape
    kv = keys.shape[1]
    grouped = queries.reshape(tok, kv, heads // kv, hd)
    scores = jnp.einsum(
        "tgqd,tgpd->tgqp", grouped, keys, preferred_element_type=F32
    ) / math.sqrt(hd)
    attn_weights = jax.nn.softmax(scores, axis=-1).astype(BF16)
    context = jnp.einsum("tgqp,tgpd->tgqd", attn_weights, values, preferred_element_type=F32)
    return context.astype(BF16).reshape(tok, heads * hd)


PARTS = 4


def hidden_units(rows_ref, gain_ref, wg0_ref, wu0_ref, wg1_ref, wu1_ref, act_ref, held, scaled, sems):
    _, count, thin = rows_ref.shape
    features, hid = wg0_ref.shape
    part = features // PARTS
    copies = []
    for i in range(PARTS):
        for j, ref in enumerate((wg1_ref, wu1_ref)):
            copies.append(
                pltpu.make_async_copy(
                    ref.at[pl.ds(i * part, part), :],
                    held.at[pl.ds(i * part, part), pl.ds(j * hid, hid)],
                    sems.at[i, j],
                )
            )
    for copy in copies:
        copy.start()
    step = 2 * thin
    steps = features // step
    own = jnp.zeros((count, 2 * hid), F32)
    squares = jnp.zeros((count, step), F32)
    for at in range(steps):
        core, pair = divmod(at, steps // NC)
        first = 2 * pair * NC + core
        here = slice(at * step, (at + 1) * step)
        rows = jnp.concatenate([rows_ref[first], rows_ref[first + NC]], axis=1).astype(F32)
        squares = squares + rows * rows
        normed = (rows * gain_ref[:, here]).astype(BF16)
        scaled[:, here] = normed
        weights = jnp.concatenate([wg0_ref[here, :], wu0_ref[here, :]], axis=1)
        own = own + jnp.dot(normed, weights, preferred_element_type=F32)
    other = jnp.zeros((count, 2 * hid), F32)
    for at in range(steps):
        if at % (steps // PARTS) == 0:
            i = at // (steps // PARTS)
            copies[2 * i].wait()
            copies[2 * i + 1].wait()
        here = slice(at * step, (at + 1) * step)
        other = other + jnp.dot(scaled[:, here], held[here, :], preferred_element_type=F32)
    inv = lax.rsqrt(jnp.sum(squares, axis=1, keepdims=True) / features + 1e-06)
    for i, both in enumerate((own, other)):
        gate = both[:, :hid] * inv
        up = both[:, hid:] * inv
        act_ref[:, i * hid : (i + 1) * hid] = (gate / (1.0 + jnp.exp(-gate)) * up).astype(BF16)


def hidden_acts(features, gain, w_gate, w_up, gate_other, up_other):
    _, count, _ = features.shape
    d_model, hid = w_gate.shape
    vmem, far = pl.BlockSpec(memory_space=pltpu.VMEM), pl.BlockSpec(memory_space=pltpu.HBM)
    return pl.pallas_call(
        hidden_units,
        out_shape=jax.ShapeDtypeStruct((count, NC * hid), BF16),
        in_specs=[vmem] * 4 + [far] * 2,
        out_specs=vmem,
        scratch_shapes=[
            pltpu.VMEM((d_model, 2 * hid), BF16),
            pltpu.VMEM((count, d_model), BF16),
            pltpu.SemaphoreType.DMA((PARTS, 2)),
        ],
        compiler_params=pltpu.CompilerParams(vmem_limit_bytes=24 * 1024 * 1024),
    )(features, gain, w_gate, w_up, gate_other, up_other)


def down_rows(own_ref, other_ref, wd0_ref, wd1_ref, wd2_ref, wd3_ref, out_ref):
    core, yhi = lax.axis_index("core"), lax.axis_index("yhi")
    _, half, units = own_ref.shape
    total = jnp.zeros(out_ref.shape, F32)
    for step, wd_ref in enumerate((wd0_ref, wd1_ref, wd2_ref, wd3_ref)):
        y = lax.rem(yhi + NY - step, NY)
        other = jnp.concatenate([other_ref[y, :, units // 2 :], other_ref[y, :, : units // 2]], 1)
        act = jnp.concatenate([own_ref[y], other], axis=0)
        weights = wd_ref[...].reshape(units, out_ref.shape[1])
        total = total + jnp.dot(act, weights, preferred_element_type=F32)
    for flip in range(NC):
        at = pl.multiple_of(lax.rem(core + flip, NC) * half, half)
        out_ref[pl.ds(at, half), :] = total[flip * half : (flip + 1) * half].astype(BF16)


def project(h_ref, w_ref, out_ref):
    cols, _, thin = out_ref.shape
    half = cols // NC
    for core in range(NC):
        for p in range(0, half, 2):
            at = (core * half + p) * thin
            both = jnp.dot(
                h_ref[...], w_ref[:, at : at + 2 * thin], preferred_element_type=F32
            ).astype(BF16)
            out_ref[p * NC + core] = both[:, :thin]
            out_ref[(p + 1) * NC + core] = both[:, thin:]


def cut_features(w_ref, same_ref, other_ref):
    core, yhi = lax.axis_index("core"), lax.axis_index("yhi")
    thin = same_ref.shape[2] // NX
    for flip, ref in enumerate((same_ref, other_ref)):
        c = lax.rem(core + flip, NC)
        for step in range(NY):
            y = lax.rem(yhi + step, NY)
            for x in range(NX):
                at = pl.multiple_of(((c * NX + x) * NY + y) * thin, thin)
                ref[step, :, x * thin : (x + 1) * thin] = w_ref[:, pl.ds(at, thin)]


def spread(in_ref, out_ref):
    rows, slots, thin = in_ref.shape
    per, half = slots // NX, rows // NC
    for x in range(NX):
        for core in range(NC):
            part = in_ref[core * half : (core + 1) * half, x * per : (x + 1) * per, :]
            part = part.reshape(half * per, thin)
            for y in range(NY):
                out_ref[(x * NY + y) * NC + core] = part


def join(in_ref, hidden_ref, out_ref):
    _, _, wide = in_ref.shape
    thin = wide // NX
    for y in range(NY):
        for core in range(NC):
            total = in_ref[y * NC + core].astype(F32)
            for x in range(1, NX):
                total = total + in_ref[(x * NY + y) * NC + core].astype(F32)
            for x in range(NX):
                at = ((core * NX + x) * NY + y) * thin
                here = slice(at, at + thin)
                done = total[:, x * thin : (x + 1) * thin] + hidden_ref[:, here].astype(F32)
                out_ref[:, here] = done.astype(BF16)


def local_call(body, outs, n_in):
    vmem = pl.BlockSpec(memory_space=pltpu.VMEM)
    out_shape = [jax.ShapeDtypeStruct(shape, BF16) for shape in outs]
    single = len(outs) == 1
    return pl.pallas_call(
        body,
        out_shape=out_shape[0] if single else out_shape,
        in_specs=[vmem] * n_in,
        out_specs=vmem if single else [vmem] * len(outs),
        compiler_params=pltpu.CompilerParams(vmem_limit_bytes=24 * 1024 * 1024),
    )


def shards(
    hidden, queries, keys, values, out_proj, norm_gain, routes, route_probs, w_gate, w_up, w_down
):
    rows = lax.axis_size("row")
    x, yhi, core = lax.axis_index("x"), lax.axis_index("yhi"), lax.axis_index("core")
    col_id = (x * NY + yhi) * NC + core
    tok_dev = queries.shape[0]
    block, d_model = hidden.shape
    cols = NX * NY * NC
    thin = d_model // cols
    wide = d_model // (NY * NC)
    count = rows * CAP

    route_weight = (route_probs / jnp.sum(route_probs, axis=-1, keepdims=True)).astype(BF16)
    earlier = (jnp.arange(block)[:, None] < jnp.arange(block)[None, :]).astype(BF16)
    slots = jnp.arange(CAP, dtype=F32)

    def slotted(experts):
        match = routes.T[None, :, :] == experts[:, None, None]
        hits = jnp.any(match, axis=1)
        before = jnp.dot(hits.astype(BF16), earlier, preferred_element_type=F32)
        place = hits[:, None, :] & (before[:, None, :] == slots[None, :, None])
        return match, place.astype(BF16)

    _, place = slotted(jnp.arange(rows * NX, dtype=jnp.int32))
    place = place.reshape(rows * NX * CAP, block)
    match, mine = slotted(jnp.arange(rows, dtype=jnp.int32) * NX + x)
    chosen = jnp.sum(jnp.where(match, route_weight.T[None], jnp.zeros((), BF16)), axis=1)
    combine = (mine * chosen[:, None, :]).reshape(count, block).T

    gate_other, up_other = swap_cores(w_gate), swap_cores(w_up)

    context = attention(queries, keys, values)
    heads_out = jnp.moveaxis(context.reshape(tok_dev, cols, -1), 1, 0)
    head_rows = exchange(heads_out, COL).reshape(block, -1)

    part = local_call(project, [(cols, block, thin)], 2)(head_rows, out_proj)
    part = exchange(part, COL)
    attn = jnp.sum(part.astype(F32), axis=0)
    own_at = ((core * NX + x) * NY + yhi) * thin
    place, hidden_part = lax.optimization_barrier(
        (place, lax.dynamic_slice_in_dim(hidden, own_at, thin, 1))
    )
    resid = hidden_part.astype(F32) + attn

    outgoing = jnp.dot(place, resid.astype(BF16), preferred_element_type=F32).astype(BF16)
    arrived = exchange(outgoing.reshape(rows, NX * CAP, thin), "row")

    hid = w_down.shape[0]
    same, rest = local_call(cut_features, [(NY, hid, wide)] * 2, 1)(w_down)
    rest = swap_cores(rest)
    pieces = [jnp.stack(pair) for pair in zip(same, rest)]
    down = [pieces[0]] + [turn(pieces[step], step) for step in (1, 3, 2)]
    down = [down[0], down[1], down[3], down[2]]

    by_expert = local_call(spread, [(cols, count // NC, thin)], 1)(arrived)
    features = exchange(by_expert, COL)
    act = hidden_acts(
        features, norm_gain.reshape(1, d_model), w_gate, w_up, gate_other, up_other
    )
    own_act = to_all(act, "yhi", NY)
    other_act = swap_cores(own_act)
    back = local_call(down_rows, [(count, wide)], 6)(own_act, other_act, *down)
    returned = exchange(back.reshape(rows, CAP, wide), "row").reshape(count, wide)

    own_hidden = lax.dynamic_slice_in_dim(hidden, col_id * tok_dev, tok_dev, 0)
    own_hidden, returned = lax.optimization_barrier((own_hidden, returned))

    attn_here = jnp.concatenate([jnp.where(x == i, attn, 0.0) for i in range(NX)], axis=1)
    mixed = jnp.dot(combine, returned, preferred_element_type=F32) + attn_here
    final = exchange(mixed.astype(BF16).reshape(cols, tok_dev, wide), COL)
    return local_call(join, [(tok_dev, d_model)], 2)(final, own_hidden)


def solution(mesh):
    rows = mesh.shape["row"]
    fine = Mesh(mesh.devices.reshape(rows, NX, NY, NC), ("row",) + COL)
    every = ("row",) + COL
    return jax.shard_map(
        shards,
        mesh=fine,
        in_specs=(
            P("row", None),
            P(every, None, None),
            P(every, None, None, None),
            P(every, None, None, None),
            P(COL, None),
            P(),
            P("row", None),
            P("row", None),
            P(None, every),
            P(None, every),
            P(every, None),
        ),
        out_specs=P(every, None),
        check_vma=False,
    )
```
